32 devices in a mesh: section: 4 (over y, x), fsdp: 8 (over z, core).
Axes of the slice: x: 2, y: 2, z: 4, core: 2. Of those that a mesh axis runs over, the one named last changes fastest.
Arguments:
- patches: bfloat16 [8, 1024, 768], P(None, 'fsdp'), may hold values from -6 to 6
- cotangent: bfloat16 [8, 1024, 768], P(None, 'fsdp'), may hold values from -6 to 6
- embed_blocks: int32 [8], replicated, may hold values from 4 to 6
- ratio_index: int32 [8], replicated, may hold values from 0 to 2
- depth: int32 [8], replicated, may hold values from 2 to 4
- w_up: bfloat16 [4, 768, 3072], P('section', 'fsdp'), may hold values from -0.21875 to 0.21875
- w_down: bfloat16 [4, 3072, 768], P('section', 'fsdp'), may hold values from -0.109375 to 0.109375
- ln_gain: bfloat16 [4, 768], P('section', 'fsdp'), may hold values from 0.099609375 to 1.8984375
Outputs:
- grad_up: float32 [4, 768, 3072], P('section', 'fsdp')
- grad_down: float32 [4, 3072, 768], P('section', 'fsdp')
- grad_gain: float32 [4, 768], P('section', 'fsdp')
The draws below stay inside these ranges and needn't reach their ends.
All inputs are finite; a program needn't handle non-finite values.
Results may differ from the reference program's by a relative error of at most 0.028.
Values may be sent and summed in bfloat16 or wider, within the bound.
A program may use at most 192 MiB of HBM per device.

```python
import jax
import jax.numpy as jnp
from jax import lax

D = 768
FF = 3072
BLOCK = 128
MICRO = 8
LAYERS = 4
TOKENS = 1024
N_SECTION = 4


def plant(values, stream_key, low, top_value):
    longest = values.shape.index(max(values.shape))
    spots = []
    for shift in (0, 1):
        where = [jax.random.randint(jax.random.fold_in(stream_key, axis), (), 0, length) for axis, length in enumerate(values.shape)]
        where[longest] = (where[longest] + shift) % values.shape[longest]
        spots.append(tuple(where))
    return values.at[spots[0]].set(low).at[spots[1]].set(top_value)


def strengthened(entries, own_key, source, target, blocks, factor):
    def block_of(position):
        return (jnp.arange(entries.shape[position]) // (entries.shape[position] // blocks)).reshape((-1,) + (1,) * (entries.ndim - 1 - position))

    first = jax.random.permutation(own_key, blocks)[block_of(target)]
    far = (block_of(target) + blocks // 2) % blocks
    return jnp.where((block_of(source) == first) | (block_of(source) == far), factor * entries, entries)


def level_of(stream_key, dims, split, least, high):
    gain = 1.0
    for axis_at, parts in split:
        steps = jax.random.uniform(jax.random.fold_in(jax.random.fold_in(stream_key, 6), axis_at), (parts,), jnp.float32, least / len(split), high / len(split))
        gain = gain * jnp.repeat(jnp.exp(steps), dims[axis_at] // parts).reshape((-1,) + (1,) * (len(dims) - 1 - axis_at))
    return gain


def scatter_about(rng, extent, spread, limit, cuts=(), dtype=jnp.bfloat16):
    values = jax.random.normal(rng, extent, jnp.float32) * spread
    if len(cuts) > 0:
        values = level_of(rng, extent, cuts, -0.22, 0.18) * values
    return jnp.clip(values, min=-limit, max=limit).astype(dtype)


def bell_draw_with(rng, shape, scale, bound, shards, heavy, dtype=jnp.bfloat16):
    entries = scale * jax.random.normal(rng, shape, jnp.float32)
    if shards:
        entries = entries * level_of(rng, shape, shards, -0.22, 0.18)
    return jnp.clip(strengthened(entries, jax.random.fold_in(rng, 3), *heavy), -bound, bound).astype(dtype)


def setup_inputs(seed: int = 0) -> dict:
    seeds = jax.random.split(jax.random.key(seed), 9)
    return {
        "patches": scatter_about(seeds[0], (MICRO, TOKENS, D), 1.0, 6.0, ((1, 8),)),
        "cotangent": bell_draw_with(seeds[1], (MICRO, TOKENS, D), 1.0, 6.0, ((1, 8),), (1, 2, 8, 2.0)),
        "embed_blocks": plant(jax.random.randint(seeds[2], (MICRO,), D // BLOCK - 2, D // BLOCK + 1), jax.random.fold_in(seeds[2], 1), D // BLOCK - 2, (D // BLOCK + 1) - 1).astype(jnp.int32),
        "ratio_index": plant(jax.random.randint(seeds[3], (MICRO,), 0, 3), jax.random.fold_in(seeds[3], 1), 0, 2).astype(jnp.int32),
        "depth": plant(jax.random.randint(seeds[4], (MICRO,), N_SECTION - 2, N_SECTION + 1), jax.random.fold_in(seeds[4], 1), N_SECTION - 2, N_SECTION).astype(jnp.int32),
        "w_up": scatter_about(seeds[5], (LAYERS, D, FF), D ** -0.5, 0.21875, ((0, 4), (1, 8))),
        "w_down": scatter_about(seeds[6], (LAYERS, FF, D), FF ** -0.5, 0.109375, ((0, 4), (1, 8))),
        "ln_gain": jnp.clip(1.0 + 0.18 * jax.random.normal(seeds[7], (LAYERS, D), jnp.float32), 0.099609375, 1.8984375).astype(jnp.bfloat16),
    }


EPSILON = 1e-05

def micro_masks(blocks, ratio, feature_count, hidden_count):
    width_int = (blocks * BLOCK).astype(jnp.int32)
    hidden_int = (width_int * (6 + ratio) // 2).astype(jnp.int32)
    embed_mask = (lax.iota(jnp.int32, feature_count) < width_int).astype(jnp.float32)
    hidden_mask = (lax.iota(jnp.int32, hidden_count) < hidden_int).astype(jnp.float32)
    return (embed_mask, hidden_mask, width_int.astype(jnp.float32))

def layer_norm(inputs, embed_mask, width_float):
    values = inputs.astype(jnp.float32) * embed_mask
    center_value = lax.optimization_barrier(jnp.sum(values, axis=-1, keepdims=True)) / width_float
    centered = (values - center_value) * embed_mask
    variance = lax.optimization_barrier(jnp.sum(centered * centered, axis=-1, keepdims=True)) / width_float
    inv_std = lax.rsqrt(variance + EPSILON)
    return (centered * inv_std, inv_std)

def layer_forward(inputs, gain_vector, weight_up, weight_down, embed_mask, hidden_mask, active, width_float):
    standard, inv_std = layer_norm(inputs, embed_mask, width_float)
    normed = (standard * gain_vector.astype(jnp.float32)).astype(jnp.bfloat16)
    hidden = jnp.dot(normed, weight_up, preferred_element_type=jnp.float32)
    activated = (jax.nn.gelu(hidden) * hidden_mask).astype(jnp.bfloat16)
    branch = jnp.dot(activated, weight_down, preferred_element_type=jnp.float32)
    output = (inputs.astype(jnp.float32) + active * embed_mask * branch).astype(jnp.bfloat16)
    return (output, hidden)

def layer_backward(inputs, hidden, grad_out, gain_vector, weight_up, weight_down, embed_mask, hidden_mask, active, width_float):
    standard, inv_std = layer_norm(inputs, embed_mask, width_float)
    gain_float = gain_vector.astype(jnp.float32)
    normed = (standard * gain_float).astype(jnp.bfloat16)
    activated = (jax.nn.gelu(hidden) * hidden_mask).astype(jnp.bfloat16)
    grad_branch = (active * embed_mask * grad_out.astype(jnp.float32)).astype(jnp.bfloat16)
    grad_act = lax.dot_general(grad_branch, weight_down, (((1,), (1,)), ((), ())), preferred_element_type=jnp.float32)
    unused, pullback = jax.vjp(jax.nn.gelu, hidden)
    grad_hidden = pullback(grad_act * hidden_mask)[0].astype(jnp.bfloat16)
    grad_normed = lax.dot_general(grad_hidden, weight_up, (((1,), (1,)), ((), ())), preferred_element_type=jnp.float32)
    grad_standard = grad_normed * gain_float * embed_mask
    grad_gain = lax.optimization_barrier(jnp.sum(grad_normed * standard, axis=0))
    first_mean = lax.optimization_barrier(jnp.sum(grad_standard, axis=-1, keepdims=True)) / width_float
    second_mean = lax.optimization_barrier(jnp.sum(grad_standard * standard, axis=-1, keepdims=True)) / width_float
    grad_norm_in = inv_std * (grad_standard - first_mean * embed_mask - standard * second_mean)
    grad_in = (grad_out.astype(jnp.float32) + grad_norm_in).astype(jnp.bfloat16)
    return (grad_in, normed, grad_hidden, activated, grad_branch, grad_gain)

def contract_rows(left, right):
    return lax.dot_general(left, right, (((0,), (0,)), ((), ())), preferred_element_type=jnp.float32)

def reference(patches, cotangent, embed_blocks, ratio_index, depth, w_up, w_down, ln_gain):
    feature_count = w_up.shape[1]
    hidden_count = w_up.shape[2]
    grads_up = [jnp.zeros((feature_count, hidden_count), jnp.float32) for layer_number in range(LAYERS)]
    grads_down = [jnp.zeros((hidden_count, feature_count), jnp.float32) for layer_number in range(LAYERS)]
    grads_gain = [jnp.zeros((feature_count,), jnp.float32) for layer_number in range(LAYERS)]
    for micro_number in range(MICRO):
        embed_mask, hidden_mask, width_float = micro_masks(embed_blocks[micro_number], ratio_index[micro_number], feature_count, hidden_count)
        inputs = (patches[micro_number].astype(jnp.float32) * embed_mask).astype(jnp.bfloat16)
        saved = []
        for layer_number in range(LAYERS):
            active = (layer_number < depth[micro_number]).astype(jnp.float32)
            output, hidden = layer_forward(inputs, ln_gain[layer_number], w_up[layer_number], w_down[layer_number], embed_mask, hidden_mask, active, width_float)
            saved.append((inputs, hidden, active))
            inputs = output
        grad_out = (cotangent[micro_number].astype(jnp.float32) * embed_mask).astype(jnp.bfloat16)
        for layer_number in reversed(range(LAYERS)):
            layer_in, hidden, active = saved[layer_number]
            grad_in, normed, grad_hidden, activated, grad_branch, grad_gain = layer_backward(layer_in, hidden, grad_out, ln_gain[layer_number], w_up[layer_number], w_down[layer_number], embed_mask, hidden_mask, active, width_float)
            grads_up[layer_number] = grads_up[layer_number] + contract_rows(normed, grad_hidden)
            grads_down[layer_number] = grads_down[layer_number] + contract_rows(activated, grad_branch)
            grads_gain[layer_number] = grads_gain[layer_number] + grad_gain
            grad_out = grad_in
    return (jnp.stack(grads_up), jnp.stack(grads_down), jnp.stack(grads_gain))
```

```python
import jax
import jax.numpy as jnp
from jax import lax
from jax.sharding import PartitionSpec as P

BLOCK = 128


EPSILON = 1e-05


def passed_along(block, axis, distance):
    devices = range(lax.axis_size(axis))
    route = [(i - distance, i) for i in devices if i - distance in devices]
    return lax.ppermute(block, axis, route)


def micro_masks(blocks, ratio, feature_count, hidden_count):
    width_int = blocks * BLOCK
    hidden_int = width_int * (6 + ratio) // 2
    embed_mask = (lax.iota(jnp.int32, feature_count) < width_int).astype(jnp.float32)
    hidden_mask = (lax.iota(jnp.int32, hidden_count) < hidden_int).astype(jnp.float32)
    return (embed_mask, hidden_mask, width_int.astype(jnp.float32))


def layer_norm(inputs, embed_mask, width_float):
    values = inputs.astype(jnp.float32) * embed_mask
    center_value = jnp.sum(values, axis=-1, keepdims=True) / width_float
    centered = (values - center_value) * embed_mask
    variance = jnp.sum(centered * centered, axis=-1, keepdims=True) / width_float
    inv_std = lax.rsqrt(variance + EPSILON)
    return (centered * inv_std, inv_std)


def run_ticks(total, tick, carry):
    for number in range(total):
        carry = tick(number, carry)
    return carry


def gelu_and_slope(hidden):
    square = hidden * hidden
    scale = 0.7978845608028654
    tanh = jnp.tanh(scale * hidden * (1.0 + 0.044715 * square))
    half = 0.5 * (1.0 + tanh)
    slope = half + (0.5 * scale) * hidden * (1.0 - tanh * tanh) * (1.0 + 0.134145 * square)
    return (hidden * half, slope)


def contract_rows(left, right):
    return lax.dot_general(
        left, right, (((0,), (0,)), ((), ())), preferred_element_type=jnp.float32
    )


def contract_last(left, right):
    return lax.dot_general(
        left, right, (((1,), (1,)), ((), ())), preferred_element_type=jnp.float32
    )


def store_row(stash, value, slot):
    return lax.dynamic_update_index_in_dim(stash, value, slot, 0)


HOP_TICKS = 2
EXTRA_ROWS = 16


def per_device(patches, cotangent, embed_blocks, ratio_index, depth, w_up, w_down, ln_gain):
    section_count = lax.axis_size("section")
    section_index = lax.axis_index("section")
    shard_count = lax.axis_size("fsdp")
    micro_count, row_count, feature_count = patches.shape
    hidden_count = w_up.shape[2]
    down_rows = w_down.shape[1]
    gain_count = ln_gain.shape[1]
    tick_total = micro_count + HOP_TICKS * (section_count - 1)
    bf16 = jnp.bfloat16

    gain_rows = jnp.pad(ln_gain, ((0, EXTRA_ROWS - 1), (0, feature_count - gain_count)))
    packed_down = jnp.concatenate([w_down[0], gain_rows], axis=0)
    weight_up = lax.all_gather(w_up[0], "fsdp", axis=0, tiled=True)
    gathered_down = lax.all_gather(packed_down, "fsdp", axis=0, tiled=True)
    gathered_down = gathered_down.reshape(shard_count, down_rows + EXTRA_ROWS, feature_count)
    weight_down = gathered_down[:, :down_rows].reshape(hidden_count, feature_count)
    gain = gathered_down[:, down_rows, :gain_count].reshape(feature_count).astype(jnp.float32)

    def masks_of(micro_index):
        is_valid = jnp.logical_and(micro_index >= 0, micro_index < micro_count)
        safe_index = jnp.clip(micro_index, 0, micro_count - 1)
        slot = jnp.where(is_valid, micro_index, micro_count)
        embed_mask, hidden_mask, width_float = micro_masks(
            embed_blocks[safe_index], ratio_index[safe_index], feature_count, hidden_count
        )
        active = (section_index < depth[safe_index]).astype(jnp.float32)
        return (safe_index, slot, is_valid, embed_mask, hidden_mask, active, width_float)

    def forward_tick(tick, carry):
        previous, incoming, stash_in, stash_act, stash_slope = carry
        sent = passed_along(previous, "section", 1)
        safe, slot, is_valid, embed_mask, hidden_mask, active, width = masks_of(
            tick - HOP_TICKS * section_index
        )
        first_in = (patches[safe].astype(jnp.float32) * embed_mask).astype(bf16)
        inputs = jnp.where(section_index == 0, first_in, incoming)
        standard, inv_std = layer_norm(inputs, embed_mask, width)
        normed = (standard * gain).astype(bf16)
        hidden = jnp.dot(normed, weight_up, preferred_element_type=jnp.float32)
        value, slope = gelu_and_slope(hidden)
        act = (value * hidden_mask).astype(bf16)
        slope = (slope * hidden_mask).astype(bf16)
        branch = jnp.dot(act, weight_down, preferred_element_type=jnp.float32)
        output = (inputs.astype(jnp.float32) + active * embed_mask * branch).astype(bf16)
        return (
            output,
            sent,
            store_row(stash_in, inputs, slot),
            store_row(stash_act, act, slot),
            store_row(stash_slope, slope, slot),
        )

    def empty(width):
        return jnp.zeros((micro_count + 1, row_count, width), bf16)

    nothing = jnp.zeros((row_count, feature_count), bf16)
    carry = (nothing, nothing, empty(feature_count), empty(hidden_count), empty(hidden_count))
    carry = run_ticks(tick_total, forward_tick, carry)
    unused_out, unused_sent, stash_in, stash_act, stash_slope = carry

    def backward_tick(tick, carry):
        previous, incoming, acc_gain, stash_branch, stash_hidden, stash_normed = carry
        sent = passed_along(previous, "section", -1)
        safe, slot, is_valid, embed_mask, hidden_mask, active, width = masks_of(
            tick - HOP_TICKS * (section_count - 1 - section_index)
        )
        last_in = (cotangent[safe].astype(jnp.float32) * embed_mask).astype(bf16)
        grad_out = jnp.where(section_index == section_count - 1, last_in, incoming)
        grad_float = grad_out.astype(jnp.float32)
        live = jnp.where(is_valid, active, 0.0)
        grad_branch = (live * embed_mask * grad_float).astype(bf16)
        grad_act = contract_last(grad_branch, weight_down)
        grad_hidden = (grad_act * stash_slope[slot].astype(jnp.float32)).astype(bf16)
        grad_normed = contract_last(grad_hidden, weight_up)
        standard, inv_std = layer_norm(stash_in[slot], embed_mask, width)
        normed = (standard * gain).astype(bf16)
        grad_standard = grad_normed * gain * embed_mask
        acc_gain = acc_gain + jnp.sum(grad_normed * standard, axis=0)
        first_mean = jnp.sum(grad_standard, axis=-1, keepdims=True) / width
        second_mean = jnp.sum(grad_standard * standard, axis=-1, keepdims=True) / width
        grad_norm_in = inv_std * (grad_standard - first_mean * embed_mask - standard * second_mean)
        grad_in = (grad_float + grad_norm_in).astype(bf16)
        return (
            grad_in,
            sent,
            acc_gain,
            store_row(stash_branch, grad_branch, slot),
            store_row(stash_hidden, grad_hidden, slot),
            store_row(stash_normed, normed, slot),
        )

    carry = (
        nothing,
        nothing,
        jnp.zeros((feature_count,), jnp.float32),
        empty(feature_count),
        empty(hidden_count),
        empty(feature_count),
    )
    carry = run_ticks(tick_total, backward_tick, carry)
    unused_out, unused_sent, acc_gain, stash_branch, stash_hidden, stash_normed = carry

    def flat(stash):
        return stash.reshape(-1, stash.shape[-1])

    part_down = contract_rows(flat(stash_act), flat(stash_branch)).astype(bf16)
    part_gain = acc_gain.astype(bf16).reshape(shard_count, 1, gain_count)
    part_gain = jnp.pad(
        part_gain, ((0, 0), (0, EXTRA_ROWS - 1), (0, feature_count - gain_count))
    )
    packed = jnp.concatenate(
        [part_down.reshape(shard_count, down_rows, feature_count), part_gain], axis=1
    ).reshape(-1, feature_count)
    own_down = lax.psum_scatter(packed, "fsdp", scatter_dimension=0, tiled=True)
    part_up = contract_rows(flat(stash_normed), flat(stash_hidden)).astype(bf16)
    own_up = lax.psum_scatter(part_up, "fsdp", scatter_dimension=0, tiled=True)
    grad_up = own_up.astype(jnp.float32)[None]
    grad_down = own_down[:down_rows].astype(jnp.float32)[None]
    grad_gain = own_down[down_rows, :gain_count].astype(jnp.float32)[None]
    return (grad_up, grad_down, grad_gain)


def solution(mesh):
    return jax.shard_map(
        per_device,
        mesh=mesh,
        in_specs=(
            P(None, "fsdp", None),
            P(None, "fsdp", None),
            P(),
            P(),
            P(),
            P("section", "fsdp", None),
            P("section", "fsdp", None),
            P("section", "fsdp"),
        ),
        out_specs=(P("section", "fsdp", None), P("section", "fsdp", None), P("section", "fsdp")),
        check_vma=False,
    )
```
